128 devices in a mesh: dp: 1, tp2: 64 (over z, y, x), tp: 2 (over core).
Axes of the slice: x: 4, y: 4, z: 4, core: 2. Of those that a mesh axis runs over, the one named last changes fastest.
Arguments:
- attn_out: bfloat16 [8192, 8192], P('dp', 'tp')
- w_out: bfloat16 [8192, 8192], P('tp', 'tp2')
- residual: bfloat16 [8192, 8192], P(('dp', 'tp'), 'tp2')
- norm_gain: float32 [8192], P('tp2')
Outputs:
- output 1: bfloat16 [8192, 8192], P(('dp', 'tp'), 'tp2')
- output 2: bfloat16 [8192, 8192], P(('dp', 'tp'), 'tp2')
All inputs are finite; a program needn't handle non-finite values.
Results may differ from the reference program's by a relative error of at most 0.00667563.
Values are sent between devices in bfloat16 or wider.
A program may use at most 1 GiB of HBM per device.

```python
import jax
import jax.numpy as jnp
from jax import lax

TOKENS = 8192
D = 8192
HEADS = 32
HEAD = 256
TP = 2
EPS_NORM = 1e-6


def setup_inputs(seed: int = 0, part: int = 0) -> dict:
    attn_width = HEADS * HEAD
    root_key = jax.random.key(seed)
    key_attn, key_w, key_res, key_gain = jax.random.split(root_key, 4)
    attn_vals = jax.random.normal(jax.random.fold_in(key_attn, part), (TOKENS, attn_width), jnp.float32)
    w_vals = jax.random.normal(key_w, (attn_width, D), jnp.float32) * (attn_width ** -0.5)
    res_vals = jax.random.normal(jax.random.fold_in(key_res, part), (TOKENS, D), jnp.float32)
    gain_vals = 1.0 + 0.3 * jax.random.normal(key_gain, (D,), jnp.float32)
    return {"attn_out": attn_vals.astype(jnp.bfloat16), "w_out": w_vals.astype(jnp.bfloat16), "residual": res_vals.astype(jnp.bfloat16), "norm_gain": gain_vals}


def reference(attn_out, w_out, residual, norm_gain):
    attn_width = attn_out.shape[1]
    shard_cols = attn_width // TP
    attn_shards = attn_out.reshape(TOKENS, TP, shard_cols).transpose(1, 0, 2)
    w_shards = w_out.reshape(TP, shard_cols, D)

    def add_shard(running, shard_pair):
        attn_blk, w_blk = shard_pair
        block_prod = jnp.dot(attn_blk, w_blk, preferred_element_type=jnp.float32).astype(jnp.bfloat16)
        return running + block_prod.astype(jnp.float32), None

    y_sum, _ = lax.scan(add_shard, jnp.zeros((TOKENS, D), jnp.float32), (attn_shards, w_shards))
    hidden = residual.astype(jnp.float32) + y_sum
    mean_sq = jnp.mean(hidden * hidden, axis=-1, keepdims=True)
    normed = hidden * lax.rsqrt(mean_sq + EPS_NORM) * norm_gain
    return hidden.astype(jnp.bfloat16), normed.astype(jnp.bfloat16)
```

```python
import functools
import itertools

import jax
import jax.numpy as jnp
from jax import lax
from jax.experimental import pallas as pl
from jax.experimental.pallas import tpu as pltpu
from jax.sharding import PartitionSpec as P

EPS_NORM = 1e-6
MESH = pl.DeviceIdType.MESH
F32, BF16 = jnp.float32, jnp.bfloat16

T = 256
NB = 6
AHEAD = 4
HEAD = 2
BARRIER_AT = 5
EPI_FROM = 8
GROUPS = 4
SIDE = 4


def ring_distance(d):
    return min(d, SIDE - d)


OFFSETS = sorted(
    (o for o in itertools.product(range(SIDE), repeat=3) if any(o)),
    key=lambda o: -sum(map(ring_distance, o)),
)
PEERS = len(OFFSETS)


def kernel(a, w, res, gain, h_out, n_out, abuf, wbuf, rbuf, gbuf, sendbuf, recvbuf, ybuf, hbuf, sq, parts,
           a_sem, w_sem, r_sem, g_sem, psend_sem, precv_sem, qsend_sem, qrecv_sem):
    core = lax.axis_index("tp")
    me = lax.axis_index("tp2")
    z, y, x = me // (SIDE * SIDE), (me // SIDE) % SIDE, me % SIDE
    own_rows = h_out.shape[0]
    n = own_rows // T
    width = w.shape[1] * (PEERS + 1)
    rows128 = own_rows // 128 // GROUPS
    chunks = n // GROUPS

    def peer(o):
        return {"tp2": ((z + o[0]) % SIDE) * (SIDE * SIDE) + ((y + o[1]) % SIDE) * SIDE + (x + o[2]) % SIDE}

    partner = {"tp": 1 - core}

    def chunk_row(q):
        if isinstance(q, int):
            mine, j = (False, 0) if q == 0 else (True, n - 1) if q == 2 * n - 1 else (q % 2 == 0, (q - 1) // 2 + (q % 2))
            half = core if mine else 1 - core
        else:
            first, last, even = q == 0, q == 2 * n - 1, q % 2 == 0
            mine = jnp.logical_and(jnp.logical_or(even, last), jnp.logical_not(first))
            j = jnp.where(first, 0, jnp.where(last, n - 1, (q - 1) // 2 + q % 2))
            half = jnp.where(mine, core, 1 - core)
        return pl.multiple_of(half * own_rows + j * T, T)

    def a_copy(q):
        slot = q % NB
        return pltpu.make_async_copy(a.at[pl.ds(chunk_row(q), T)], abuf.at[slot], a_sem.at[slot])

    w_copy = pltpu.make_async_copy(w, wbuf, w_sem)
    r_copy = pltpu.make_async_copy(res, rbuf, r_sem)
    g_copy = pltpu.make_async_copy(gain, gbuf, g_sem)

    w_copy.start()
    for q in range(HEAD):
        a_copy(q).start()

    barrier = pltpu.get_barrier_semaphore()
    for o in OFFSETS:
        pl.semaphore_signal(barrier, inc=1, device_id=peer(o), device_id_type=MESH)
    pl.semaphore_signal(barrier, inc=1, device_id=partner, device_id_type=MESH)

    def rows_of(j):
        return pl.ds(pl.multiple_of(j * T, T), T)

    def partner_copy(first, count):
        rows = pl.ds(pl.multiple_of(first * T, T), count * T)
        return pltpu.make_async_remote_copy(
            src_ref=sendbuf.at[rows], dst_ref=recvbuf.at[rows], send_sem=psend_sem.at[first], recv_sem=precv_sem.at[first],
            device_id=partner, device_id_type=MESH,
        )

    def finish_h(e, group):
        rows = rows_of(e)
        total = ybuf[rows, :].astype(F32) + recvbuf[rows, :].astype(F32)
        h = rbuf[rows, :].astype(F32) + total
        hbuf[rows, :] = h
        h_out[rows, :] = h.astype(BF16)
        squares = h * h
        for b in range(T // 128):
            block = jnp.transpose(squares[b * 128:(b + 1) * 128, :])
            sq[group, pl.ds((e % chunks) * (T // 128) + b, 1), :] = jnp.sum(block, axis=0, keepdims=True)

    def send_squares(group):
        parts[group, me] = sq[group]
        for o in OFFSETS:
            pltpu.make_async_remote_copy(
                src_ref=sq.at[group], dst_ref=parts.at[group, me], send_sem=qsend_sem.at[group],
                recv_sem=qrecv_sem.at[group], device_id=peer(o), device_id_type=MESH,
            ).start()

    def wait_squares(group, sem):
        pltpu.make_async_copy(parts.at[group, pl.ds(0, PEERS)], parts.at[group, pl.ds(0, PEERS)], sem.at[group]).wait()

    def finish_n(group):
        wait_squares(group, qrecv_sem)
        inv = lax.rsqrt(jnp.sum(parts[group], axis=0) / width + EPS_NORM)
        g = gbuf[...]
        for i in range(rows128):
            rows = pl.ds((group * rows128 + i) * 128, 128)
            scale = jnp.transpose(jnp.broadcast_to(inv[i:i + 1, :], (128, 128)))
            n_out[rows, :] = (hbuf[rows, :] * scale * g).astype(BF16)

    def main():
        def product(q):
            slot = q % NB
            a_copy(q).wait()
            return slot

        def take(slot):
            return jnp.dot(abuf[slot], wbuf[...], preferred_element_type=F32).astype(BF16)

        def request(q):
            if isinstance(q, int):
                if q < 2 * n:
                    a_copy(q).start()
            else:
                @pl.when(q < 2 * n)
                def _():
                    a_copy(q).start()

        w_copy.wait()
        for q in range(HEAD, AHEAD + 1):
            request(q)
        slot = product(0)
        sendbuf[rows_of(0), :] = take(slot)
        r_copy.start()
        g_copy.start()

        def step(j, extra):
            request(2 * j + AHEAD + 1)
            request(2 * j + AHEAD + 2)
            theirs = product(2 * j + 1)
            mine = product(2 * j + 2)
            sendbuf[rows_of(j + 1), :] = take(theirs)
            ybuf[rows_of(j), :] = take(mine)
            extra()

        def loop(low, high, extra=lambda j: None, after=lambda j: None):
            def body(j, _):
                step(j, lambda: extra(j))
                after(j)
                return 0

            lax.fori_loop(low, high, body, 0)

        loop(0, BARRIER_AT + 1)
        pl.semaphore_wait(barrier, PEERS + 1)
        first = BARRIER_AT + 2
        partner_copy(0, first).start()

        def send(j):
            partner_copy(j + 1, 1).start()

        loop(BARRIER_AT + 1, EPI_FROM, after=send)
        partner_copy(0, first).wait_recv()
        r_copy.wait()
        g_copy.wait()

        e = 0
        j = EPI_FROM
        while j < n - 1:
            group = e // chunks
            steps = min(chunks // 2, n - 1 - j)

            def extra(jj, base=e - 2 * j, group=group):
                for b in range(2):
                    e_now = base + 2 * jj + b
                    if True:
                        finish_h(e_now, group)

            if e >= first or e + 2 * steps > first:
                inner = extra

                def extra(jj, inner=inner, base=e - 2 * j):
                    for b in range(2):
                        e_now = base + 2 * jj + b

                        @pl.when(e_now >= first)
                        def _():
                            partner_copy(e_now, 1).wait_recv()

                    inner(jj)

            loop(j, j + steps, extra=extra, after=send)
            j += steps
            e += 2 * steps
            if e % chunks == 0:
                send_squares(e // chunks - 1)

        slot = product(2 * n - 1)
        ybuf[rows_of(n - 1), :] = take(slot)
        while e < n - 1:
            partner_copy(e, 1).wait_recv()
            finish_h(e, e // chunks)
            e += 1
        partner_copy(n - 1, 1).wait_recv()
        finish_h(n - 1, GROUPS - 1)
        send_squares(GROUPS - 1)
        for group in range(GROUPS):
            finish_n(group)
        partner_copy(0, first).wait_send()
        for j in range(first, n):
            partner_copy(j, 1).wait_send()
        for group in range(GROUPS):
            wait_squares(group, qsend_sem)

    main()


def solution(mesh):
    def local_step(attn_blk, w_blk, res_blk, gain_blk):
        rows, cols = res_blk.shape
        n = rows // T
        rows128 = rows // 128 // GROUPS
        hbm = pl.BlockSpec(memory_space=pltpu.HBM)
        vmem = pl.BlockSpec(memory_space=pltpu.VMEM)
        out = jax.ShapeDtypeStruct((rows, cols), BF16)
        return pl.pallas_call(
            kernel,
            out_shape=(out, out),
            in_specs=[hbm] * 4,
            out_specs=(vmem, vmem),
            scratch_shapes=[
                pltpu.VMEM((NB, T, attn_blk.shape[1]), BF16),
                pltpu.VMEM(w_blk.shape, BF16),
                pltpu.VMEM((rows, cols), BF16),
                pltpu.VMEM((1, cols), F32),
                pltpu.VMEM((rows, cols), BF16),
                pltpu.VMEM((rows, cols), BF16),
                pltpu.VMEM((rows, cols), BF16),
                pltpu.VMEM((rows, cols), F32),
                pltpu.VMEM((GROUPS, rows128, 128), F32),
                pltpu.VMEM((GROUPS, PEERS + 1, rows128, 128), F32),
                pltpu.SemaphoreType.DMA((NB,)),
                pltpu.SemaphoreType.DMA,
                pltpu.SemaphoreType.DMA,
                pltpu.SemaphoreType.DMA,
                pltpu.SemaphoreType.DMA((n,)),
                pltpu.SemaphoreType.DMA((n,)),
                pltpu.SemaphoreType.DMA((GROUPS,)),
                pltpu.SemaphoreType.DMA((GROUPS,)),
            ],
            compiler_params=pltpu.CompilerParams(collective_id=0, has_side_effects=True, vmem_limit_bytes=40 * 2**20),
        )(*(pltpu.with_memory_space_constraint(v, pltpu.HBM) for v in (attn_blk, w_blk, res_blk, gain_blk.reshape(1, cols))))

    row_spec = P(("dp", "tp"), "tp2")
    return jax.shard_map(
        local_step, mesh=mesh, in_specs=(P("dp", "tp"), P("tp", "tp2"), row_spec, P("tp2")),
        out_specs=(row_spec, row_spec), check_vma=False,
    )
```

```python
import itertools

import jax
import jax.numpy as jnp
from jax import lax
from jax.experimental import pallas as pl
from jax.experimental.pallas import tpu as pltpu
from jax.sharding import PartitionSpec as P

EPS_NORM = 1e-6
MESH = pl.DeviceIdType.MESH
F32, BF16 = jnp.float32, jnp.bfloat16

T = 256
NB = 8
AHEAD = 6
HEAD = 2
BARRIER_AT = 4
EPI_FROM = 7
STAGED = (8, 5)
SIDE = 4
OUT_PARTS = 2


def ring_distance(d):
    return min(d, SIDE - d)


OFFSETS = sorted(
    (o for o in itertools.product(range(SIDE), repeat=3) if any(o)),
    key=lambda o: -sum(map(ring_distance, o)),
)
PEERS = len(OFFSETS)
STAGES = tuple(tuple(tuple(d if i == axis else 0 for i in range(3)) for d in (2, 1, 3)) for axis in (2, 1, 0))


def kernel(a, w, res, gain, h_out, n_out, abuf, wbuf, rbuf, gbuf, sendbuf, recvbuf, ybuf, hbuf, last_sq, last_parts, *rest):
    n_staged = len(STAGED)
    staged_sq, staged_parts, rest = rest[:n_staged], rest[n_staged:2 * n_staged], rest[2 * n_staged:]
    a_sem, w_sem, r_sem, g_sem, psend_sem, precv_sem, qsend_sem, qrecv_sem, ssend_sem, srecv_sem = rest
    core = lax.axis_index("tp")
    me = lax.axis_index("tp2")
    z, y, x = me // (SIDE * SIDE), (me // SIDE) % SIDE, me % SIDE
    own_rows = h_out.shape[0]
    n = own_rows // T
    per = T // 128
    width = w.shape[1] * (PEERS + 1)

    def peer(o):
        return {"tp2": ((z + o[0]) % SIDE) * (SIDE * SIDE) + ((y + o[1]) % SIDE) * SIDE + (x + o[2]) % SIDE}

    partner = {"tp": 1 - core}

    def chunk_row(q):
        if isinstance(q, int):
            mine, j = (False, 0) if q == 0 else (True, n - 1) if q == 2 * n - 1 else (q % 2 == 0, (q - 1) // 2 + (q % 2))
            half = core if mine else 1 - core
        else:
            first, last, even = q == 0, q == 2 * n - 1, q % 2 == 0
            mine = jnp.logical_and(jnp.logical_or(even, last), jnp.logical_not(first))
            j = jnp.where(first, 0, jnp.where(last, n - 1, (q - 1) // 2 + q % 2))
            half = jnp.where(mine, core, 1 - core)
        return pl.multiple_of(half * own_rows + j * T, T)

    def a_copy(q):
        slot = q % NB
        return pltpu.make_async_copy(a.at[pl.ds(chunk_row(q), T)], abuf.at[slot], a_sem.at[slot])

    w_copy = pltpu.make_async_copy(w, wbuf, w_sem)
    r_copy = pltpu.make_async_copy(res, rbuf, r_sem)
    g_copy = pltpu.make_async_copy(gain, gbuf, g_sem)

    w_copy.start()
    for q in range(HEAD):
        a_copy(q).start()

    barrier = pltpu.get_barrier_semaphore()
    for o in OFFSETS:
        pl.semaphore_signal(barrier, inc=1, device_id=peer(o), device_id_type=MESH)
    pl.semaphore_signal(barrier, inc=1, device_id=partner, device_id_type=MESH)

    def rows_of(j):
        return pl.ds(pl.multiple_of(j * T, T), T)

    def partner_copy(first, count):
        rows = pl.ds(pl.multiple_of(first * T, T), count * T)
        return pltpu.make_async_remote_copy(
            src_ref=sendbuf.at[rows], dst_ref=recvbuf.at[rows], send_sem=psend_sem.at[first], recv_sem=precv_sem.at[first],
            device_id=partner, device_id_type=MESH,
        )

    def finish_h(e, sums, at):
        rows = rows_of(e)
        total = ybuf[rows, :].astype(F32) + recvbuf[rows, :].astype(F32)
        h = rbuf[rows, :].astype(F32) + total
        hbuf[rows, :] = h
        h_out[rows, :] = h.astype(BF16)
        squares = h * h
        for b in range(per):
            block = jnp.transpose(squares[b * 128:(b + 1) * 128, :])
            sums[pl.ds(at * per + b, 1), :] = jnp.sum(block, axis=0, keepdims=True)

    def send_stage(group, stage):
        parts = staged_parts[group]
        here = (x, y, z)[stage]
        parts[stage, here] = staged_sq[group][stage]
        for o in STAGES[stage]:
            pltpu.make_async_remote_copy(
                src_ref=staged_sq[group].at[stage], dst_ref=parts.at[stage, here], send_sem=ssend_sem.at[group, stage],
                recv_sem=srecv_sem.at[group, stage], device_id=peer(o), device_id_type=MESH,
            ).start()

    def wait_stage(group, stage, sem):
        whole = staged_parts[group].at[stage, pl.ds(0, SIDE - 1)]
        pltpu.make_async_copy(whole, whole, sem.at[group, stage]).wait()

    def next_stage(group, stage):
        wait_stage(group, stage - 1, srecv_sem)
        staged_sq[group][stage] = jnp.sum(staged_parts[group][stage - 1], axis=0)
        send_stage(group, stage)

    def staged_sums(group):
        wait_stage(group, len(STAGES) - 1, srecv_sem)
        return jnp.sum(staged_parts[group][len(STAGES) - 1], axis=0)

    def send_last():
        for o in OFFSETS:
            pltpu.make_async_remote_copy(
                src_ref=last_sq, dst_ref=last_parts.at[me], send_sem=qsend_sem, recv_sem=qrecv_sem,
                device_id=peer(o), device_id_type=MESH,
            ).start()
        last_parts[me] = last_sq[...]

    def wait_last(sem):
        whole = last_parts.at[pl.ds(0, PEERS)]
        pltpu.make_async_copy(whole, whole, sem).wait()

    def finish_n(first, sums):
        inv = lax.rsqrt(sums / width + EPS_NORM)
        g = gbuf[...]
        for i in range(sums.shape[0]):
            rows = pl.ds(first * T + i * 128, 128)
            scale = jnp.transpose(jnp.broadcast_to(inv[i:i + 1, :], (128, 128)))
            n_out[rows, :] = (hbuf[rows, :] * scale * g).astype(BF16)

    def request(q):
        if isinstance(q, int):
            if q < 2 * n:
                a_copy(q).start()
        else:
            @pl.when(q < 2 * n)
            def _():
                a_copy(q).start()

    def product(q):
        return jnp.dot(abuf[q % NB], wbuf[...], preferred_element_type=F32).astype(BF16)

    def loop(low, high, before=lambda j: None, after=lambda j: None):
        def body(j, _):
            request(2 * j + AHEAD + 1)
            request(2 * j + AHEAD + 2)
            a_copy(2 * j + 1).wait()
            a_copy(2 * j + 2).wait()
            before(j)
            sendbuf[rows_of(j + 1), :] = product(2 * j + 1)
            ybuf[rows_of(j), :] = product(2 * j + 2)
            after(j)
            return 0

        lax.fori_loop(low, high, body, 0)

    w_copy.wait()
    for q in range(HEAD, AHEAD + 1):
        request(q)
    a_copy(0).wait()
    sendbuf[rows_of(0), :] = product(0)
    r_copy.start()
    g_copy.start()
    loop(0, BARRIER_AT + 1)

    pl.semaphore_wait(barrier, PEERS + 1)
    first = BARRIER_AT + 2
    partner_copy(0, first).start()

    def send(j):
        partner_copy(j + 1, 1).start()

    loop(BARRIER_AT + 1, EPI_FROM, after=send)
    partner_copy(0, first).wait_recv()
    r_copy.wait()
    g_copy.wait()

    ends = [sum(STAGED[:i + 1]) for i in range(n_staged)]

    def place(e):
        for group, end in enumerate(ends):
            if e < end:
                return staged_sq[group].at[0], end - STAGED[group]
        return last_sq, ends[-1]

    def events(done):
        for group, end in enumerate(ends):
            if done == end:
                send_stage(group, 0)

    e, j = 0, EPI_FROM
    stage_of = [None] * n_staged
    while j < n - 1:
        count = 2 if e + 2 <= j else 1
        sums, base = place(e)
        steps = 1
        while (
            j + steps < n - 1 and (2 if e + count * steps + 2 <= j + steps else 1) == count
            and place(e + count * steps)[1] == base and e + count * steps not in ends
            and (e >= first) == (e + count * steps >= first)
        ):
            steps += 1

        def before(jj, e=e, j=j, count=count, sums=sums, base=base):
            for b in range(count):
                now = e + (jj - j) * count + b
                if e + b >= first:
                    partner_copy(now, 1).wait_recv()
                elif e + b + (steps - 1) * count >= first:
                    @pl.when(now >= first)
                    def _():
                        partner_copy(now, 1).wait_recv()
                finish_h(now, sums, now - base)

        loop(j, j + steps, before=before, after=send)
        e += count * steps
        j += steps
        for group in range(n_staged):
            if stage_of[group] is not None and stage_of[group][0] < 1 and j - stage_of[group][1] >= 3:
                next_stage(group, 1)
                stage_of[group] = (1, j)
        for group, end in enumerate(ends):
            if e == end:
                send_stage(group, 0)
                stage_of[group] = (0, j)

    while e < n - 1:
        partner_copy(e, 1).wait_recv()
        sums, base = place(e)
        finish_h(e, sums, e - base)
        e += 1
    a_copy(2 * n - 1).wait()
    ybuf[rows_of(n - 1), :] = product(2 * n - 1)
    partner_copy(n - 1, 1).wait_recv()
    finish_h(n - 1, last_sq, n - 1 - ends[-1])
    send_last()

    for stage in range(1, len(STAGES)):
        for group in range(n_staged):
            if stage > stage_of[group][0]:
                next_stage(group, stage)
    for group, end in enumerate(ends):
        finish_n(end - STAGED[group], staged_sums(group))
    partner_copy(0, first).wait_send()
    for j in range(first, n):
        partner_copy(j, 1).wait_send()
    for group in range(n_staged):
        for stage in range(len(STAGES)):
            wait_stage(group, stage, ssend_sem)
    wait_last(qsend_sem)
    wait_last(qrecv_sem)
    finish_n(ends[-1], jnp.sum(last_parts[...], axis=0))


def write_kernel(h, n, h_out, n_out, sem):
    copies = []
    rows = h.shape[0] // OUT_PARTS
    for i, (src, dst) in enumerate(((h, h_out), (n, n_out))):
        for k in range(OUT_PARTS):
            part = pl.ds(k * rows, rows)
            copies.append(pltpu.make_async_copy(src.at[part], dst.at[part], sem.at[i, k]))
    for copy in copies:
        copy.start()
    for copy in copies:
        copy.wait()


def solution(mesh):
    def local_step(attn_blk, w_blk, res_blk, gain_blk):
        rows, cols = res_blk.shape
        n = rows // T
        per = T // 128
        last = (n - sum(STAGED)) * per
        hbm = pl.BlockSpec(memory_space=pltpu.HBM)
        vmem = pl.BlockSpec(memory_space=pltpu.VMEM)
        out = jax.ShapeDtypeStruct((rows, cols), BF16)
        h, normed = pl.pallas_call(
            kernel,
            out_shape=(out, out),
            in_specs=[hbm] * 4,
            out_specs=(vmem, vmem),
            scratch_shapes=[
                pltpu.VMEM((NB, T, attn_blk.shape[1]), BF16),
                pltpu.VMEM(w_blk.shape, BF16),
                pltpu.VMEM((rows, cols), BF16),
                pltpu.VMEM((1, cols), F32),
                pltpu.VMEM((rows, cols), BF16),
                pltpu.VMEM((rows, cols), BF16),
                pltpu.VMEM((rows, cols), BF16),
                pltpu.VMEM((rows, cols), F32),
                pltpu.VMEM((last, 128), F32),
                pltpu.VMEM((PEERS + 1, last, 128), F32),
                *(pltpu.VMEM((len(STAGES), c * per, 128), F32) for c in STAGED),
                *(pltpu.VMEM((len(STAGES), SIDE, c * per, 128), F32) for c in STAGED),
                pltpu.SemaphoreType.DMA((NB,)),
                pltpu.SemaphoreType.DMA,
                pltpu.SemaphoreType.DMA,
                pltpu.SemaphoreType.DMA,
                pltpu.SemaphoreType.DMA((n,)),
                pltpu.SemaphoreType.DMA((n,)),
                pltpu.SemaphoreType.DMA,
                pltpu.SemaphoreType.DMA,
                pltpu.SemaphoreType.DMA((len(STAGED), len(STAGES))),
                pltpu.SemaphoreType.DMA((len(STAGED), len(STAGES))),
            ],
            compiler_params=pltpu.CompilerParams(collective_id=0, has_side_effects=True, vmem_limit_bytes=40 * 2**20),
        )(*(pltpu.with_memory_space_constraint(v, pltpu.HBM) for v in (attn_blk, w_blk, res_blk, gain_blk.reshape(1, cols))))
        return pl.pallas_call(
            write_kernel,
            out_shape=(out, out),
            in_specs=[vmem] * 2,
            out_specs=(hbm, hbm),
            scratch_shapes=[pltpu.SemaphoreType.DMA((2, OUT_PARTS))],
            compiler_params=pltpu.CompilerParams(vmem_limit_bytes=16 * 2**20),
        )(h, normed)

    row_spec = P(("dp", "tp"), "tp2")
    return jax.shard_map(
        local_step, mesh=mesh, in_specs=(P("dp", "tp"), P("tp", "tp2"), row_spec, P("tp2")),
        out_specs=(row_spec, row_spec), check_vma=False,
    )
```

```python
import itertools

import jax
import jax.numpy as jnp
from jax import lax
from jax.experimental import pallas as pl
from jax.experimental.pallas import tpu as pltpu
from jax.sharding import PartitionSpec as P

EPS_NORM = 1e-6
MESH = pl.DeviceIdType.MESH
F32, BF16 = jnp.float32, jnp.bfloat16

T = 256
NB = 8
AHEAD = 6
HEAD = 2
BARRIER_AT = 4
EPI_FROM = 7
STAGED = ((8, ((2,), (1,), (0,))), (5, ((1, 2), (0,))))
SIDE = 4
OUT_PARTS = 2


def ring_distance(d):
    return min(d, SIDE - d)


OFFSETS = sorted(
    (o for o in itertools.product(range(SIDE), repeat=3) if any(o)),
    key=lambda o: -sum(map(ring_distance, o)),
)
PEERS = len(OFFSETS)


def stage_offsets(axes):
    return [o for o in OFFSETS if all(o[i] == 0 for i in range(3) if i not in axes)]


def kernel(a, w, res, gain, h_out, n_out, abuf, wbuf, rbuf, gbuf, sendbuf, recvbuf, ybuf, hbuf, last_sq, last_parts, *rest):
    n_staged = len(STAGED)
    staged_sq, staged_parts, rest = rest[:n_staged], rest[n_staged:2 * n_staged], rest[2 * n_staged:]
    a_sem, w_sem, r_sem, g_sem, psend_sem, precv_sem, qsend_sem, qrecv_sem, ssend_sem, srecv_sem = rest
    core = lax.axis_index("tp")
    me = lax.axis_index("tp2")
    z, y, x = me // (SIDE * SIDE), (me // SIDE) % SIDE, me % SIDE
    own_rows = h_out.shape[0]
    n = own_rows // T
    per = T // 128
    width = w.shape[1] * (PEERS + 1)

    def peer(o):
        return {"tp2": ((z + o[0]) % SIDE) * (SIDE * SIDE) + ((y + o[1]) % SIDE) * SIDE + (x + o[2]) % SIDE}

    partner = {"tp": 1 - core}

    def chunk_row(q):
        if isinstance(q, int):
            mine, j = (False, 0) if q == 0 else (True, n - 1) if q == 2 * n - 1 else (q % 2 == 0, (q - 1) // 2 + (q % 2))
            half = core if mine else 1 - core
        else:
            first, last, even = q == 0, q == 2 * n - 1, q % 2 == 0
            mine = jnp.logical_and(jnp.logical_or(even, last), jnp.logical_not(first))
            j = jnp.where(first, 0, jnp.where(last, n - 1, (q - 1) // 2 + q % 2))
            half = jnp.where(mine, core, 1 - core)
        return pl.multiple_of(half * own_rows + j * T, T)

    def a_copy(q):
        slot = q % NB
        return pltpu.make_async_copy(a.at[pl.ds(chunk_row(q), T)], abuf.at[slot], a_sem.at[slot])

    w_copy = pltpu.make_async_copy(w, wbuf, w_sem)
    r_copy = pltpu.make_async_copy(res, rbuf, r_sem)
    g_copy = pltpu.make_async_copy(gain, gbuf, g_sem)

    w_copy.start()
    for q in range(HEAD):
        a_copy(q).start()

    barrier = pltpu.get_barrier_semaphore()
    for o in OFFSETS:
        pl.semaphore_signal(barrier, inc=1, device_id=peer(o), device_id_type=MESH)
    pl.semaphore_signal(barrier, inc=1, device_id=partner, device_id_type=MESH)

    def rows_of(j):
        return pl.ds(pl.multiple_of(j * T, T), T)

    def partner_copy(first, count):
        rows = pl.ds(pl.multiple_of(first * T, T), count * T)
        return pltpu.make_async_remote_copy(
            src_ref=sendbuf.at[rows], dst_ref=recvbuf.at[rows], send_sem=psend_sem.at[first], recv_sem=precv_sem.at[first],
            device_id=partner, device_id_type=MESH,
        )

    def finish_h(e, sums, at):
        rows = rows_of(e)
        total = ybuf[rows, :].astype(F32) + recvbuf[rows, :].astype(F32)
        h = rbuf[rows, :].astype(F32) + total
        hbuf[rows, :] = h
        h_out[rows, :] = h.astype(BF16)
        squares = h * h
        for b in range(per):
            block = jnp.transpose(squares[b * 128:(b + 1) * 128, :])
            sums[pl.ds(at * per + b, 1), :] = jnp.sum(block, axis=0, keepdims=True)

    def send_stage(group, stage):
        axes = STAGED[group][1][stage]
        here = 0
        for axis in axes:
            here = here * SIDE + (z, y, x)[axis]
        parts = staged_parts[group]
        for o in stage_offsets(axes):
            pltpu.make_async_remote_copy(
                src_ref=staged_sq[group].at[stage], dst_ref=parts.at[stage, here], send_sem=ssend_sem.at[group, stage],
                recv_sem=srecv_sem.at[group, stage], device_id=peer(o), device_id_type=MESH,
            ).start()
        parts[stage, here] = staged_sq[group][stage]

    def wait_stage(group, stage, sem):
        whole = staged_parts[group].at[stage, pl.ds(0, SIDE ** len(STAGED[group][1][stage]) - 1)]
        pltpu.make_async_copy(whole, whole, sem.at[group, stage]).wait()

    def stage_sums(group, stage):
        return jnp.sum(staged_parts[group][stage, 0:SIDE ** len(STAGED[group][1][stage])], axis=0)

    def next_stage(group, stage):
        wait_stage(group, stage - 1, srecv_sem)
        staged_sq[group][stage] = stage_sums(group, stage - 1)
        send_stage(group, stage)

    def staged_sums(group):
        stage = len(STAGED[group][1]) - 1
        wait_stage(group, stage, srecv_sem)
        return stage_sums(group, stage)

    def send_last():
        for o in OFFSETS:
            pltpu.make_async_remote_copy(
                src_ref=last_sq, dst_ref=last_parts.at[me], send_sem=qsend_sem, recv_sem=qrecv_sem,
                device_id=peer(o), device_id_type=MESH,
            ).start()
        last_parts[me] = last_sq[...]

    def wait_last(sem):
        whole = last_parts.at[pl.ds(0, PEERS)]
        pltpu.make_async_copy(whole, whole, sem).wait()

    def finish_n(first, sums):
        inv = lax.rsqrt(sums / width + EPS_NORM)
        g = gbuf[...]
        for i in range(sums.shape[0]):
            rows = pl.ds(first * T + i * 128, 128)
            scale = jnp.transpose(jnp.broadcast_to(inv[i:i + 1, :], (128, 128)))
            n_out[rows, :] = (hbuf[rows, :] * scale * g).astype(BF16)

    def request(q):
        if isinstance(q, int):
            if q < 2 * n:
                a_copy(q).start()
        else:
            @pl.when(q < 2 * n)
            def _():
                a_copy(q).start()

    def product(q):
        return jnp.dot(abuf[q % NB], wbuf[...], preferred_element_type=F32).astype(BF16)

    def loop(low, high, before=lambda j: None, after=lambda j: None):
        def body(j, _):
            request(2 * j + AHEAD + 1)
            request(2 * j + AHEAD + 2)
            a_copy(2 * j + 1).wait()
            a_copy(2 * j + 2).wait()
            before(j)
            sendbuf[rows_of(j + 1), :] = product(2 * j + 1)
            ybuf[rows_of(j), :] = product(2 * j + 2)
            after(j)
            return 0

        lax.fori_loop(low, high, body, 0)

    w_copy.wait()
    for q in range(HEAD, AHEAD + 1):
        request(q)
    a_copy(0).wait()
    sendbuf[rows_of(0), :] = product(0)
    r_copy.start()
    g_copy.start()
    loop(0, BARRIER_AT + 1)

    pl.semaphore_wait(barrier, PEERS + 1)
    first = BARRIER_AT + 2
    partner_copy(0, first).start()

    def send(j):
        partner_copy(j + 1, 1).start()

    loop(BARRIER_AT + 1, EPI_FROM, after=send)
    partner_copy(0, first).wait_recv()
    r_copy.wait()
    g_copy.wait()

    ends = [sum(c for c, _ in STAGED[:i + 1]) for i in range(n_staged)]

    def place(e):
        for group, end in enumerate(ends):
            if e < end:
                return staged_sq[group].at[0], end - STAGED[group][0]
        return last_sq, ends[-1]

    e, j = 0, EPI_FROM
    stage_of = [None] * n_staged
    while j < n - 1:
        count = 2 if e + 2 <= j else 1
        sums, base = place(e)
        steps = 1
        while (
            j + steps < n - 1 and (2 if e + count * steps + 2 <= j + steps else 1) == count
            and place(e + count * steps)[1] == base and e + count * steps not in ends
            and (e >= first) == (e + count * steps >= first)
        ):
            steps += 1

        def before(jj, e=e, j=j, count=count, sums=sums, base=base):
            for b in range(count):
                now = e + (jj - j) * count + b
                if e + b >= first:
                    partner_copy(now, 1).wait_recv()
                elif e + b + (steps - 1) * count >= first:
                    @pl.when(now >= first)
                    def _():
                        partner_copy(now, 1).wait_recv()
                finish_h(now, sums, now - base)

        loop(j, j + steps, before=before, after=send)
        e += count * steps
        j += steps
        for group in range(n_staged):
            if stage_of[group] is not None and stage_of[group][0] < 1 and j - stage_of[group][1] >= 3:
                next_stage(group, 1)
                stage_of[group] = (1, j)
        for group, end in enumerate(ends):
            if e == end:
                send_stage(group, 0)
                stage_of[group] = (0, j)

    while e < n - 1:
        partner_copy(e, 1).wait_recv()
        sums, base = place(e)
        finish_h(e, sums, e - base)
        e += 1
    a_copy(2 * n - 1).wait()
    ybuf[rows_of(n - 1), :] = product(2 * n - 1)
    partner_copy(n - 1, 1).wait_recv()
    finish_h(n - 1, last_sq, n - 1 - ends[-1])
    send_last()

    for stage in range(1, max(len(stages) for _, stages in STAGED)):
        for group, (_, stages) in enumerate(STAGED):
            if stage_of[group][0] < stage < len(stages):
                next_stage(group, stage)
    for group, end in enumerate(ends):
        finish_n(end - STAGED[group][0], staged_sums(group))
    partner_copy(0, first).wait_send()
    for j in range(first, n):
        partner_copy(j, 1).wait_send()
    for group in range(n_staged):
        for stage in range(len(STAGED[group][1])):
            wait_stage(group, stage, ssend_sem)
    wait_last(qsend_sem)
    wait_last(qrecv_sem)
    finish_n(ends[-1], jnp.sum(last_parts[...], axis=0))


def write_kernel(h, n, h_out, n_out, sem):
    copies = []
    rows = h.shape[0] // OUT_PARTS
    for i, (src, dst) in enumerate(((h, h_out), (n, n_out))):
        for k in range(OUT_PARTS):
            part = pl.ds(k * rows, rows)
            copies.append(pltpu.make_async_copy(src.at[part], dst.at[part], sem.at[i, k]))
    for copy in copies:
        copy.start()
    for copy in copies:
        copy.wait()


def solution(mesh):
    def local_step(attn_blk, w_blk, res_blk, gain_blk):
        rows, cols = res_blk.shape
        n = rows // T
        per = T // 128
        last = (n - sum(c for c, _ in STAGED)) * per
        n_stages = max(len(stages) for _, stages in STAGED)
        hbm = pl.BlockSpec(memory_space=pltpu.HBM)
        vmem = pl.BlockSpec(memory_space=pltpu.VMEM)
        out = jax.ShapeDtypeStruct((rows, cols), BF16)
        h, normed = pl.pallas_call(
            kernel,
            out_shape=(out, out),
            in_specs=[hbm] * 4,
            out_specs=(vmem, vmem),
            scratch_shapes=[
                pltpu.VMEM((NB, T, attn_blk.shape[1]), BF16),
                pltpu.VMEM(w_blk.shape, BF16),
                pltpu.VMEM((rows, cols), BF16),
                pltpu.VMEM((1, cols), F32),
                pltpu.VMEM((rows, cols), BF16),
                pltpu.VMEM((rows, cols), BF16),
                pltpu.VMEM((rows, cols), BF16),
                pltpu.VMEM((rows, cols), F32),
                pltpu.VMEM((last, 128), F32),
                pltpu.VMEM((PEERS + 1, last, 128), F32),
                *(pltpu.VMEM((len(stages), c * per, 128), F32) for c, stages in STAGED),
                *(
                    pltpu.VMEM((len(stages), SIDE ** max(len(axes) for axes in stages), c * per, 128), F32)
                    for c, stages in STAGED
                ),
                pltpu.SemaphoreType.DMA((NB,)),
                pltpu.SemaphoreType.DMA,
                pltpu.SemaphoreType.DMA,
                pltpu.SemaphoreType.DMA,
                pltpu.SemaphoreType.DMA((n,)),
                pltpu.SemaphoreType.DMA((n,)),
                pltpu.SemaphoreType.DMA,
                pltpu.SemaphoreType.DMA,
                pltpu.SemaphoreType.DMA((len(STAGED), n_stages)),
                pltpu.SemaphoreType.DMA((len(STAGED), n_stages)),
            ],
            compiler_params=pltpu.CompilerParams(collective_id=0, has_side_effects=True, vmem_limit_bytes=40 * 2**20),
        )(*(pltpu.with_memory_space_constraint(v, pltpu.HBM) for v in (attn_blk, w_blk, res_blk, gain_blk.reshape(1, cols))))
        return pl.pallas_call(
            write_kernel,
            out_shape=(out, out),
            in_specs=[vmem] * 2,
            out_specs=(hbm, hbm),
            scratch_shapes=[pltpu.SemaphoreType.DMA((2, OUT_PARTS))],
            compiler_params=pltpu.CompilerParams(vmem_limit_bytes=16 * 2**20),
        )(h, normed)

    row_spec = P(("dp", "tp"), "tp2")
    return jax.shard_map(
        local_step, mesh=mesh, in_specs=(P("dp", "tp"), P("tp", "tp2"), row_spec, P("tp2")),
        out_specs=(row_spec, row_spec), check_vma=False,
    )
```

```python
import itertools

import jax
import jax.numpy as jnp
from jax import lax
from jax.experimental import pallas as pl
from jax.experimental.pallas import tpu as pltpu
from jax.sharding import PartitionSpec as P

EPS_NORM = 1e-6
MESH = pl.DeviceIdType.MESH
F32, BF16 = jnp.float32, jnp.bfloat16

T = 256
NB = 8
AHEAD = 6
HEAD = 2
BARRIER_AT = 4
EPI_FROM = 7
STAGED = ((8, ((1, 2), (0,))), (5, ((1, 2), (0,))))
STAGE_STEPS = 4
SIDE = 4
OUT_PARTS = 2


def ring_distance(d):
    return min(d, SIDE - d)


OFFSETS = sorted(
    (o for o in itertools.product(range(SIDE), repeat=3) if any(o)),
    key=lambda o: -sum(map(ring_distance, o)),
)
PEERS = len(OFFSETS)


def stage_offsets(axes):
    return [o for o in OFFSETS if all(o[i] == 0 for i in range(3) if i not in axes)]


def kernel(a, w, res, gain, h_out, n_out, abuf, wbuf, rbuf, gbuf, sendbuf, recvbuf, ybuf, hbuf, last_sq, last_parts, *rest):
    n_staged = len(STAGED)
    staged_sq, staged_parts, rest = rest[:n_staged], rest[n_staged:2 * n_staged], rest[2 * n_staged:]
    a_sem, w_sem, r_sem, g_sem, psend_sem, precv_sem, qsend_sem, qrecv_sem, ssend_sem, srecv_sem = rest
    core = lax.axis_index("tp")
    me = lax.axis_index("tp2")
    z, y, x = me // (SIDE * SIDE), (me // SIDE) % SIDE, me % SIDE
    own_rows = h_out.shape[0]
    n = own_rows // T
    per = T // 128
    width = w.shape[1] * (PEERS + 1)

    def peer(o):
        return {"tp2": ((z + o[0]) % SIDE) * (SIDE * SIDE) + ((y + o[1]) % SIDE) * SIDE + (x + o[2]) % SIDE}

    partner = {"tp": 1 - core}

    def chunk_row(q):
        if isinstance(q, int):
            if q >= 2 * n - 3:
                mine, j = True, q - n
            elif q == 2 * n - 4:
                mine, j = False, n - 1
            else:
                mine, j = q % 2 == 0 and q > 0, q // 2 + q % 2 - (1 if q % 2 == 0 and q > 0 else 0)
            half = core if mine else 1 - core
        else:
            end, swap, even = q >= 2 * n - 3, q == 2 * n - 4, q % 2 == 0
            mine = jnp.logical_or(end, jnp.logical_and(even, jnp.logical_not(swap)))
            j = jnp.where(end, q - n, jnp.where(swap, n - 1, (q - 1) // 2 + q % 2))
            half = jnp.where(mine, core, 1 - core)
        return pl.multiple_of(half * own_rows + j * T, T)

    def a_copy(q):
        slot = q % NB
        return pltpu.make_async_copy(a.at[pl.ds(chunk_row(q), T)], abuf.at[slot], a_sem.at[slot])

    w_copy = pltpu.make_async_copy(w, wbuf, w_sem)
    r_copy = pltpu.make_async_copy(res, rbuf, r_sem)
    g_copy = pltpu.make_async_copy(gain, gbuf, g_sem)

    w_copy.start()
    for q in range(HEAD):
        a_copy(q).start()

    barrier = pltpu.get_barrier_semaphore()
    for o in OFFSETS:
        pl.semaphore_signal(barrier, inc=1, device_id=peer(o), device_id_type=MESH)
    pl.semaphore_signal(barrier, inc=1, device_id=partner, device_id_type=MESH)

    def rows_of(j):
        return pl.ds(pl.multiple_of(j * T, T), T)

    def partner_copy(first, count):
        rows = pl.ds(pl.multiple_of(first * T, T), count * T)
        return pltpu.make_async_remote_copy(
            src_ref=sendbuf.at[rows], dst_ref=recvbuf.at[rows], send_sem=psend_sem.at[first], recv_sem=precv_sem.at[first],
            device_id=partner, device_id_type=MESH,
        )

    def finish_h(e, sums, at):
        rows = rows_of(e)
        total = ybuf[rows, :].astype(F32) + recvbuf[rows, :].astype(F32)
        h = rbuf[rows, :].astype(F32) + total
        hbuf[rows, :] = h
        h_out[rows, :] = h.astype(BF16)
        squares = h * h
        for b in range(per):
            block = jnp.transpose(squares[b * 128:(b + 1) * 128, :])
            sums[pl.ds(at * per + b, 1), :] = jnp.sum(block, axis=0, keepdims=True)

    def send_stage(group, stage):
        axes = STAGED[group][1][stage]
        here = 0
        for axis in axes:
            here = here * SIDE + (z, y, x)[axis]
        parts = staged_parts[group]
        for o in stage_offsets(axes):
            pltpu.make_async_remote_copy(
                src_ref=staged_sq[group].at[stage], dst_ref=parts.at[stage, here], send_sem=ssend_sem.at[group, stage],
                recv_sem=srecv_sem.at[group, stage], device_id=peer(o), device_id_type=MESH,
            ).start()
        parts[stage, here] = staged_sq[group][stage]

    def wait_stage(group, stage, sem):
        whole = staged_parts[group].at[stage, pl.ds(0, SIDE ** len(STAGED[group][1][stage]) - 1)]
        pltpu.make_async_copy(whole, whole, sem.at[group, stage]).wait()

    def stage_sums(group, stage):
        return jnp.sum(staged_parts[group][stage, 0:SIDE ** len(STAGED[group][1][stage])], axis=0)

    def next_stage(group, stage):
        wait_stage(group, stage - 1, srecv_sem)
        staged_sq[group][stage] = stage_sums(group, stage - 1)
        send_stage(group, stage)

    def staged_sums(group):
        stage = len(STAGED[group][1]) - 1
        wait_stage(group, stage, srecv_sem)
        return stage_sums(group, stage)

    def send_last():
        for o in OFFSETS:
            pltpu.make_async_remote_copy(
                src_ref=last_sq, dst_ref=last_parts.at[me], send_sem=qsend_sem, recv_sem=qrecv_sem,
                device_id=peer(o), device_id_type=MESH,
            ).start()
        last_parts[me] = last_sq[...]

    def wait_last(sem):
        whole = last_parts.at[pl.ds(0, PEERS)]
        pltpu.make_async_copy(whole, whole, sem).wait()

    def finish_n(first, sums):
        inv = lax.rsqrt(sums / width + EPS_NORM)
        g = gbuf[...]
        for i in range(sums.shape[0]):
            rows = pl.ds(first * T + i * 128, 128)
            scale = jnp.transpose(jnp.broadcast_to(inv[i:i + 1, :], (128, 128)))
            n_out[rows, :] = (hbuf[rows, :] * scale * g).astype(BF16)

    def request(q):
        if isinstance(q, int):
            if q < 2 * n:
                a_copy(q).start()
        else:
            @pl.when(q < 2 * n)
            def _():
                a_copy(q).start()

    def product(q):
        return jnp.dot(abuf[q % NB], wbuf[...], preferred_element_type=F32).astype(BF16)

    def step(j, before, *places):
        request(2 * j + AHEAD + 1)
        request(2 * j + AHEAD + 2)
        a_copy(2 * j + 1).wait()
        a_copy(2 * j + 2).wait()
        before(j)
        for i, (buffer, chunk) in enumerate(places):
            buffer[rows_of(chunk), :] = product(2 * j + 1 + i)

    def loop(low, high, before=lambda j: None, after=lambda j: None):
        def body(j, _):
            step(j, before, (sendbuf, j + 1), (ybuf, j))
            after(j)
            return 0

        lax.fori_loop(low, high, body, 0)

    w_copy.wait()
    for q in range(HEAD, AHEAD + 1):
        request(q)
    a_copy(0).wait()
    sendbuf[rows_of(0), :] = product(0)
    r_copy.start()
    g_copy.start()
    loop(0, BARRIER_AT + 1)

    pl.semaphore_wait(barrier, PEERS + 1)
    first = BARRIER_AT + 2
    partner_copy(0, first).start()

    def send(j):
        partner_copy(j + 1, 1).start()

    loop(BARRIER_AT + 1, EPI_FROM, after=send)
    partner_copy(0, first).wait_recv()
    r_copy.wait()
    g_copy.wait()

    ends = [sum(c for c, _ in STAGED[:i + 1]) for i in range(n_staged)]

    def place(e):
        for group, end in enumerate(ends):
            if e < end:
                return staged_sq[group].at[0], end - STAGED[group][0]
        return last_sq, ends[-1]

    e, j = 0, EPI_FROM
    stage_of = [None] * n_staged

    def exchange():
        for group, end in enumerate(ends):
            if stage_of[group] is not None and stage_of[group][0] < 1 and j - stage_of[group][1] >= STAGE_STEPS:
                next_stage(group, 1)
                stage_of[group] = (1, j)
            if stage_of[group] is None and e == end:
                send_stage(group, 0)
                stage_of[group] = (0, j)

    while j < n - 3:
        count = 2 if e + 2 <= j else 1
        sums, base = place(e)
        steps = 1
        while (
            j + steps < n - 3 and (2 if e + count * steps + 2 <= j + steps else 1) == count
            and place(e + count * steps)[1] == base and e + count * steps not in ends
            and (e >= first) == (e + count * steps >= first)
        ):
            steps += 1

        def before(jj, e=e, j=j, count=count, sums=sums, base=base):
            for b in range(count):
                now = e + (jj - j) * count + b
                if e + b >= first:
                    partner_copy(now, 1).wait_recv()
                elif e + b + (steps - 1) * count >= first:
                    @pl.when(now >= first)
                    def _():
                        partner_copy(now, 1).wait_recv()
                finish_h(now, sums, now - base)

        loop(j, j + steps, before=before, after=send)
        e += count * steps
        j += steps
        exchange()

    def finish_one(now):
        partner_copy(now, 1).wait_recv()
        sums, base = place(now)
        finish_h(now, sums, now - base)

    ready = e
    step(n - 3, lambda _: [finish_one(i) for i in range(ready, n - 3)], (sendbuf, n - 2), (sendbuf, n - 1))
    send(n - 3)
    send(n - 2)
    e, j = n - 3, n - 2
    exchange()
    step(n - 2, lambda _: None, (ybuf, n - 3), (ybuf, n - 2))
    j = n - 1
    exchange()
    a_copy(2 * n - 1).wait()
    finish_one(n - 3)
    finish_one(n - 2)
    ybuf[rows_of(n - 1), :] = product(2 * n - 1)
    finish_one(n - 1)
    send_last()

    for stage in range(1, max(len(stages) for _, stages in STAGED)):
        for group, (_, stages) in enumerate(STAGED):
            if stage_of[group][0] < stage < len(stages):
                next_stage(group, stage)
    for group, end in enumerate(ends):
        finish_n(end - STAGED[group][0], staged_sums(group))
    partner_copy(0, first).wait_send()
    for j in range(first, n):
        partner_copy(j, 1).wait_send()
    for group in range(n_staged):
        for stage in range(len(STAGED[group][1])):
            wait_stage(group, stage, ssend_sem)
    wait_last(qsend_sem)
    wait_last(qrecv_sem)
    finish_n(ends[-1], jnp.sum(last_parts[...], axis=0))


def write_kernel(h, n, h_out, n_out, sem):
    copies = []
    rows = h.shape[0] // OUT_PARTS
    for i, (src, dst) in enumerate(((h, h_out), (n, n_out))):
        for k in range(OUT_PARTS):
            part = pl.ds(k * rows, rows)
            copies.append(pltpu.make_async_copy(src.at[part], dst.at[part], sem.at[i, k]))
    for copy in copies:
        copy.start()
    for copy in copies:
        copy.wait()


def solution(mesh):
    def local_step(attn_blk, w_blk, res_blk, gain_blk):
        rows, cols = res_blk.shape
        n = rows // T
        per = T // 128
        last = (n - sum(c for c, _ in STAGED)) * per
        n_stages = max(len(stages) for _, stages in STAGED)
        hbm = pl.BlockSpec(memory_space=pltpu.HBM)
        vmem = pl.BlockSpec(memory_space=pltpu.VMEM)
        out = jax.ShapeDtypeStruct((rows, cols), BF16)
        h, normed = pl.pallas_call(
            kernel,
            out_shape=(out, out),
            in_specs=[hbm] * 4,
            out_specs=(vmem, vmem),
            scratch_shapes=[
                pltpu.VMEM((NB, T, attn_blk.shape[1]), BF16),
                pltpu.VMEM(w_blk.shape, BF16),
                pltpu.VMEM((rows, cols), BF16),
                pltpu.VMEM((1, cols), F32),
                pltpu.VMEM((rows, cols), BF16),
                pltpu.VMEM((rows, cols), BF16),
                pltpu.VMEM((rows, cols), BF16),
                pltpu.VMEM((rows, cols), F32),
                pltpu.VMEM((last, 128), F32),
                pltpu.VMEM((PEERS + 1, last, 128), F32),
                *(pltpu.VMEM((len(stages), c * per, 128), F32) for c, stages in STAGED),
                *(
                    pltpu.VMEM((len(stages), SIDE ** max(len(axes) for axes in stages), c * per, 128), F32)
                    for c, stages in STAGED
                ),
                pltpu.SemaphoreType.DMA((NB,)),
                pltpu.SemaphoreType.DMA,
                pltpu.SemaphoreType.DMA,
                pltpu.SemaphoreType.DMA,
                pltpu.SemaphoreType.DMA((n,)),
                pltpu.SemaphoreType.DMA((n,)),
                pltpu.SemaphoreType.DMA,
                pltpu.SemaphoreType.DMA,
                pltpu.SemaphoreType.DMA((len(STAGED), n_stages)),
                pltpu.SemaphoreType.DMA((len(STAGED), n_stages)),
            ],
            compiler_params=pltpu.CompilerParams(collective_id=0, has_side_effects=True, vmem_limit_bytes=40 * 2**20),
        )(*(pltpu.with_memory_space_constraint(v, pltpu.HBM) for v in (attn_blk, w_blk, res_blk, gain_blk.reshape(1, cols))))
        return pl.pallas_call(
            write_kernel,
            out_shape=(out, out),
            in_specs=[vmem] * 2,
            out_specs=(hbm, hbm),
            scratch_shapes=[pltpu.SemaphoreType.DMA((2, OUT_PARTS))],
            compiler_params=pltpu.CompilerParams(vmem_limit_bytes=16 * 2**20),
        )(h, normed)

    row_spec = P(("dp", "tp"), "tp2")
    return jax.shard_map(
        local_step, mesh=mesh, in_specs=(P("dp", "tp"), P("tp", "tp2"), row_spec, P("tp2")),
        out_specs=(row_spec, row_spec), check_vma=False,
    )
```

```python
import itertools

import jax
import jax.numpy as jnp
from jax import lax
from jax.experimental import pallas as pl
from jax.experimental.pallas import tpu as pltpu
from jax.sharding import PartitionSpec as P

EPS_NORM = 1e-6
MESH = pl.DeviceIdType.MESH
F32, BF16 = jnp.float32, jnp.bfloat16

T = 256
NB = 8
AHEAD = 6
HEAD = 2
BARRIER_AT = 4
EPI_FROM = 7
STAGED = ((8, ((1, 2), (0,))), (5, ((1, 2), (0,))))
STAGE_STEPS = 4
SIDE = 4


def ring_distance(d):
    return min(d, SIDE - d)


OFFSETS = sorted(
    (o for o in itertools.product(range(SIDE), repeat=3) if any(o)),
    key=lambda o: -sum(map(ring_distance, o)),
)
PEERS = len(OFFSETS)


def stage_offsets(axes):
    return [o for o in OFFSETS if all(o[i] == 0 for i in range(3) if i not in axes)]


def normalize(mean, g, h, out, h_first, out_first):
    inv = lax.rsqrt(mean + EPS_NORM)
    for i in range(mean.shape[0]):
        scale = jnp.transpose(jnp.broadcast_to(inv[i:i + 1, :], (128, 128)))
        out[pl.ds(out_first + i * 128, 128), :] = (h[pl.ds(h_first + i * 128, 128), :] * scale * g).astype(BF16)


def kernel(a, w, res, gain, h_out, n_out, h_last, sums_out, gbuf, abuf, wbuf, rbuf, sendbuf, recvbuf, ybuf, hbuf, last_sq, last_parts, *rest):
    n_staged = len(STAGED)
    staged_sq, staged_parts, rest = rest[:n_staged], rest[n_staged:2 * n_staged], rest[2 * n_staged:]
    a_sem, w_sem, r_sem, g_sem, psend_sem, precv_sem, qsend_sem, qrecv_sem, ssend_sem, srecv_sem = rest
    ends = [sum(c for c, _ in STAGED[:i + 1]) for i in range(n_staged)]
    core = lax.axis_index("tp")
    me = lax.axis_index("tp2")
    z, y, x = me // (SIDE * SIDE), (me // SIDE) % SIDE, me % SIDE
    own_rows = h_out.shape[0]
    n = own_rows // T
    per = T // 128
    width = w.shape[1] * (PEERS + 1)

    def peer(o):
        return {"tp2": ((z + o[0]) % SIDE) * (SIDE * SIDE) + ((y + o[1]) % SIDE) * SIDE + (x + o[2]) % SIDE}

    partner = {"tp": 1 - core}

    def chunk_row(q):
        if isinstance(q, int):
            if q >= 2 * n - 3:
                mine, j = True, q - n
            elif q == 2 * n - 4:
                mine, j = False, n - 1
            else:
                mine, j = q % 2 == 0 and q > 0, q // 2 + q % 2 - (1 if q % 2 == 0 and q > 0 else 0)
            half = core if mine else 1 - core
        else:
            end, swap, even = q >= 2 * n - 3, q == 2 * n - 4, q % 2 == 0
            mine = jnp.logical_or(end, jnp.logical_and(even, jnp.logical_not(swap)))
            j = jnp.where(end, q - n, jnp.where(swap, n - 1, (q - 1) // 2 + q % 2))
            half = jnp.where(mine, core, 1 - core)
        return pl.multiple_of(half * own_rows + j * T, T)

    def a_copy(q):
        slot = q % NB
        return pltpu.make_async_copy(a.at[pl.ds(chunk_row(q), T)], abuf.at[slot], a_sem.at[slot])

    w_copy = pltpu.make_async_copy(w, wbuf, w_sem)
    r_copy = pltpu.make_async_copy(res, rbuf, r_sem)
    g_copy = pltpu.make_async_copy(gain, gbuf, g_sem)

    w_copy.start()
    for q in range(HEAD):
        a_copy(q).start()

    barrier = pltpu.get_barrier_semaphore()
    for o in OFFSETS:
        pl.semaphore_signal(barrier, inc=1, device_id=peer(o), device_id_type=MESH)
    pl.semaphore_signal(barrier, inc=1, device_id=partner, device_id_type=MESH)

    def rows_of(j):
        return pl.ds(pl.multiple_of(j * T, T), T)

    def partner_copy(first, count):
        rows = pl.ds(pl.multiple_of(first * T, T), count * T)
        return pltpu.make_async_remote_copy(
            src_ref=sendbuf.at[rows], dst_ref=recvbuf.at[rows], send_sem=psend_sem.at[first], recv_sem=precv_sem.at[first],
            device_id=partner, device_id_type=MESH,
        )

    def finish_h(e, sums, at):
        rows = rows_of(e)
        total = ybuf[rows, :].astype(F32) + recvbuf[rows, :].astype(F32)
        h = rbuf[rows, :].astype(F32) + total
        if isinstance(e, int) and e >= ends[-1]:
            h_last[(e - ends[-1]) * T:(e - ends[-1] + 1) * T, :] = h
        else:
            hbuf[rows, :] = h
        h_out[rows, :] = h.astype(BF16)
        squares = h * h
        for b in range(per):
            block = jnp.transpose(squares[b * 128:(b + 1) * 128, :])
            sums[pl.ds(at * per + b, 1), :] = jnp.sum(block, axis=0, keepdims=True)

    def send_stage(group, stage):
        axes = STAGED[group][1][stage]
        here = 0
        for axis in axes:
            here = here * SIDE + (z, y, x)[axis]
        parts = staged_parts[group]
        for o in stage_offsets(axes):
            pltpu.make_async_remote_copy(
                src_ref=staged_sq[group].at[stage], dst_ref=parts.at[stage, here], send_sem=ssend_sem.at[group, stage],
                recv_sem=srecv_sem.at[group, stage], device_id=peer(o), device_id_type=MESH,
            ).start()
        parts[stage, here] = staged_sq[group][stage]

    def wait_stage(group, stage, sem):
        whole = staged_parts[group].at[stage, pl.ds(0, SIDE ** len(STAGED[group][1][stage]) - 1)]
        pltpu.make_async_copy(whole, whole, sem.at[group, stage]).wait()

    def stage_sums(group, stage):
        return jnp.sum(staged_parts[group][stage, 0:SIDE ** len(STAGED[group][1][stage])], axis=0)

    def next_stage(group, stage):
        wait_stage(group, stage - 1, srecv_sem)
        staged_sq[group][stage] = stage_sums(group, stage - 1)
        send_stage(group, stage)

    def staged_sums(group):
        stage = len(STAGED[group][1]) - 1
        wait_stage(group, stage, srecv_sem)
        return stage_sums(group, stage)

    def send_last():
        for o in OFFSETS:
            pltpu.make_async_remote_copy(
                src_ref=last_sq, dst_ref=last_parts.at[me], send_sem=qsend_sem, recv_sem=qrecv_sem,
                device_id=peer(o), device_id_type=MESH,
            ).start()
        last_parts[me] = last_sq[...]

    def wait_last(sem):
        whole = last_parts.at[pl.ds(0, PEERS)]
        pltpu.make_async_copy(whole, whole, sem).wait()

    def finish_n(first, sums):
        normalize(sums / width, gbuf[...], hbuf, n_out, first * T, first * T)

    def request(q):
        if isinstance(q, int):
            if q < 2 * n:
                a_copy(q).start()
        else:
            @pl.when(q < 2 * n)
            def _():
                a_copy(q).start()

    def product(q):
        return jnp.dot(abuf[q % NB], wbuf[...], preferred_element_type=F32).astype(BF16)

    def step(j, before, *places):
        request(2 * j + AHEAD + 1)
        request(2 * j + AHEAD + 2)
        a_copy(2 * j + 1).wait()
        a_copy(2 * j + 2).wait()
        before(j)
        for i, (buffer, chunk) in enumerate(places):
            buffer[rows_of(chunk), :] = product(2 * j + 1 + i)

    def loop(low, high, before=lambda j: None, after=lambda j: None):
        def body(j, _):
            step(j, before, (sendbuf, j + 1), (ybuf, j))
            after(j)
            return 0

        lax.fori_loop(low, high, body, 0)

    w_copy.wait()
    for q in range(HEAD, AHEAD + 1):
        request(q)
    a_copy(0).wait()
    sendbuf[rows_of(0), :] = product(0)
    r_copy.start()
    g_copy.start()
    loop(0, BARRIER_AT + 1)

    pl.semaphore_wait(barrier, PEERS + 1)
    first = BARRIER_AT + 2
    partner_copy(0, first).start()

    def send(j):
        partner_copy(j + 1, 1).start()

    loop(BARRIER_AT + 1, EPI_FROM, after=send)
    partner_copy(0, first).wait_recv()
    r_copy.wait()
    g_copy.wait()


    def place(e):
        for group, end in enumerate(ends):
            if e < end:
                return staged_sq[group].at[0], end - STAGED[group][0]
        return last_sq, ends[-1]

    e, j = 0, EPI_FROM
    stage_of = [None] * n_staged

    def exchange():
        for group, end in enumerate(ends):
            if stage_of[group] is not None and stage_of[group][0] < 1 and j - stage_of[group][1] >= STAGE_STEPS:
                next_stage(group, 1)
                stage_of[group] = (1, j)
            if stage_of[group] is None and e == end:
                send_stage(group, 0)
                stage_of[group] = (0, j)

    while j < n - 3:
        count = 2 if e + 2 <= j else 1
        sums, base = place(e)
        steps = 1
        while (
            j + steps < n - 3 and (2 if e + count * steps + 2 <= j + steps else 1) == count
            and place(e + count * steps)[1] == base and e + count * steps not in ends
            and (e >= first) == (e + count * steps >= first)
        ):
            steps += 1

        def before(jj, e=e, j=j, count=count, sums=sums, base=base):
            for b in range(count):
                now = e + (jj - j) * count + b
                if e + b >= first:
                    partner_copy(now, 1).wait_recv()
                elif e + b + (steps - 1) * count >= first:
                    @pl.when(now >= first)
                    def _():
                        partner_copy(now, 1).wait_recv()
                finish_h(now, sums, now - base)

        loop(j, j + steps, before=before, after=send)
        e += count * steps
        j += steps
        exchange()

    def finish_one(now):
        partner_copy(now, 1).wait_recv()
        sums, base = place(now)
        finish_h(now, sums, now - base)

    ready = e
    step(n - 3, lambda _: [finish_one(i) for i in range(ready, n - 3)], (sendbuf, n - 2), (sendbuf, n - 1))
    send(n - 3)
    send(n - 2)
    e, j = n - 3, n - 2
    exchange()
    step(n - 2, lambda _: None, (ybuf, n - 3), (ybuf, n - 2))
    j = n - 1
    exchange()
    a_copy(2 * n - 1).wait()
    finish_one(n - 3)
    finish_one(n - 2)
    ybuf[rows_of(n - 1), :] = product(2 * n - 1)
    finish_one(n - 1)
    send_last()

    for stage in range(1, max(len(stages) for _, stages in STAGED)):
        for group, (_, stages) in enumerate(STAGED):
            if stage_of[group][0] < stage < len(stages):
                next_stage(group, stage)
    for group, end in enumerate(ends):
        finish_n(end - STAGED[group][0], staged_sums(group))
    partner_copy(0, first).wait_send()
    for j in range(first, n):
        partner_copy(j, 1).wait_send()
    for group in range(n_staged):
        for stage in range(len(STAGED[group][1])):
            wait_stage(group, stage, ssend_sem)
    wait_last(qsend_sem)
    wait_last(qrecv_sem)
    sums_out[...] = jnp.sum(last_parts[...], axis=0) / width


def write_kernel(h, n, h_last, mean, gain, h_out, n_out, last_n, sem):
    early = h.shape[0] - h_last.shape[0]
    copies = [
        pltpu.make_async_copy(n.at[pl.ds(0, early)], n_out.at[pl.ds(0, early)], sem.at[0]),
        pltpu.make_async_copy(h, h_out, sem.at[1]),
    ]
    for copy in copies:
        copy.start()
    normalize(mean[...], gain[...], h_last, last_n, 0, 0)
    copies.append(pltpu.make_async_copy(last_n, n_out.at[pl.ds(early, h_last.shape[0])], sem.at[2]))
    copies[-1].start()
    for copy in copies:
        copy.wait()


def solution(mesh):
    def local_step(attn_blk, w_blk, res_blk, gain_blk):
        rows, cols = res_blk.shape
        n = rows // T
        per = T // 128
        last = (n - sum(c for c, _ in STAGED)) * per
        n_stages = max(len(stages) for _, stages in STAGED)
        hbm = pl.BlockSpec(memory_space=pltpu.HBM)
        vmem = pl.BlockSpec(memory_space=pltpu.VMEM)
        out = jax.ShapeDtypeStruct((rows, cols), BF16)
        last_rows = jax.ShapeDtypeStruct((last * 128, cols), F32)
        finished = pl.pallas_call(
            kernel,
            out_shape=(out, out, last_rows, jax.ShapeDtypeStruct((last, 128), F32), jax.ShapeDtypeStruct((1, cols), F32)),
            in_specs=[hbm] * 4,
            out_specs=(vmem,) * 5,
            scratch_shapes=[
                pltpu.VMEM((NB, T, attn_blk.shape[1]), BF16),
                pltpu.VMEM(w_blk.shape, BF16),
                pltpu.VMEM((rows, cols), BF16),
                pltpu.VMEM((rows, cols), BF16),
                pltpu.VMEM((rows, cols), BF16),
                pltpu.VMEM((rows, cols), BF16),
                pltpu.VMEM((rows, cols), F32),
                pltpu.VMEM((last, 128), F32),
                pltpu.VMEM((PEERS + 1, last, 128), F32),
                *(pltpu.VMEM((len(stages), c * per, 128), F32) for c, stages in STAGED),
                *(
                    pltpu.VMEM((len(stages), SIDE ** max(len(axes) for axes in stages), c * per, 128), F32)
                    for c, stages in STAGED
                ),
                pltpu.SemaphoreType.DMA((NB,)),
                pltpu.SemaphoreType.DMA,
                pltpu.SemaphoreType.DMA,
                pltpu.SemaphoreType.DMA,
                pltpu.SemaphoreType.DMA((n,)),
                pltpu.SemaphoreType.DMA((n,)),
                pltpu.SemaphoreType.DMA,
                pltpu.SemaphoreType.DMA,
                pltpu.SemaphoreType.DMA((len(STAGED), n_stages)),
                pltpu.SemaphoreType.DMA((len(STAGED), n_stages)),
            ],
            compiler_params=pltpu.CompilerParams(collective_id=0, has_side_effects=True, vmem_limit_bytes=40 * 2**20),
        )(*(pltpu.with_memory_space_constraint(v, pltpu.HBM) for v in (attn_blk, w_blk, res_blk, gain_blk.reshape(1, cols))))
        return pl.pallas_call(
            write_kernel,
            out_shape=(out, out),
            in_specs=[vmem] * 5,
            out_specs=(hbm, hbm),
            scratch_shapes=[pltpu.VMEM((last * 128, cols), BF16), pltpu.SemaphoreType.DMA((3,))],
            compiler_params=pltpu.CompilerParams(vmem_limit_bytes=16 * 2**20),
        )(*finished)

    row_spec = P(("dp", "tp"), "tp2")
    return jax.shard_map(
        local_step, mesh=mesh, in_specs=(P("dp", "tp"), P("tp", "tp2"), row_spec, P("tp2")),
        out_specs=(row_spec, row_spec), check_vma=False,
    )
```

```python
import itertools

import jax
import jax.numpy as jnp
from jax import lax
from jax.experimental import pallas as pl
from jax.experimental.pallas import tpu as pltpu
from jax.sharding import PartitionSpec as P

EPS_NORM = 1e-6
MESH = pl.DeviceIdType.MESH
F32, BF16 = jnp.float32, jnp.bfloat16

T = 256
NB = 8
AHEAD = 6
HEAD = 2
BARRIER_AT = 4
EPI_FROM = 7
STAGED = ((8, ((1, 2), (0,))), (5, ((1, 2), (0,))))
STAGE_STEPS = 4
SIDE = 4


def ring_distance(d):
    return min(d, SIDE - d)


OFFSETS = sorted(
    (o for o in itertools.product(range(SIDE), repeat=3) if any(o)),
    key=lambda o: -sum(map(ring_distance, o)),
)
PEERS = len(OFFSETS)


def stage_offsets(axes):
    return [o for o in OFFSETS if all(o[i] == 0 for i in range(3) if i not in axes)]


def normalize(mean, g, h, out, h_first, out_first):
    inv = lax.rsqrt(mean + EPS_NORM)
    for i in range(mean.shape[0]):
        scale = jnp.transpose(jnp.broadcast_to(inv[i:i + 1, :], (128, 128)))
        out[pl.ds(out_first + i * 128, 128), :] = (h[pl.ds(h_first + i * 128, 128), :] * scale * g).astype(BF16)


def kernel(a, w, res, gain, h_out, n_out, h_last, sums_out, gbuf, abuf, wbuf, rbuf, sendbuf, recvbuf, ybuf, hbuf, last_sq, last_parts, *rest):
    n_staged = len(STAGED)
    staged_sq, staged_parts, rest = rest[:n_staged], rest[n_staged:2 * n_staged], rest[2 * n_staged:]
    a_sem, w_sem, r_sem, g_sem, psend_sem, precv_sem, qsend_sem, qrecv_sem, ssend_sem, srecv_sem = rest
    ends = [sum(c for c, _ in STAGED[:i + 1]) for i in range(n_staged)]
    core = lax.axis_index("tp")
    me = lax.axis_index("tp2")
    z, y, x = me // (SIDE * SIDE), (me // SIDE) % SIDE, me % SIDE
    own_rows = h_out.shape[0]
    n = own_rows // T
    per = T // 128
    width = w.shape[1] * (PEERS + 1)

    def peer(o):
        return {"tp2": ((z + o[0]) % SIDE) * (SIDE * SIDE) + ((y + o[1]) % SIDE) * SIDE + (x + o[2]) % SIDE}

    partner = {"tp": 1 - core}

    def chunk_row(q):
        if isinstance(q, int):
            if q >= 2 * n - 3:
                mine, j = True, q - n
            elif q == 2 * n - 4:
                mine, j = False, n - 1
            else:
                mine, j = q % 2 == 0 and q > 0, q // 2 + q % 2 - (1 if q % 2 == 0 and q > 0 else 0)
            half = core if mine else 1 - core
        else:
            end, swap, even = q >= 2 * n - 3, q == 2 * n - 4, q % 2 == 0
            mine = jnp.logical_or(end, jnp.logical_and(even, jnp.logical_not(swap)))
            j = jnp.where(end, q - n, jnp.where(swap, n - 1, (q - 1) // 2 + q % 2))
            half = jnp.where(mine, core, 1 - core)
        return pl.multiple_of(half * own_rows + j * T, T)

    def a_copy(q):
        slot = q % NB
        return pltpu.make_async_copy(a.at[pl.ds(chunk_row(q), T)], abuf.at[slot], a_sem.at[slot])

    w_copy = pltpu.make_async_copy(w, wbuf, w_sem)
    r_copy = pltpu.make_async_copy(res, rbuf, r_sem)
    g_copy = pltpu.make_async_copy(gain, gbuf, g_sem)

    w_copy.start()
    for q in range(HEAD):
        a_copy(q).start()

    barrier = pltpu.get_barrier_semaphore()
    for o in OFFSETS:
        pl.semaphore_signal(barrier, inc=1, device_id=peer(o), device_id_type=MESH)
    pl.semaphore_signal(barrier, inc=1, device_id=partner, device_id_type=MESH)

    def rows_of(j):
        return pl.ds(pl.multiple_of(j * T, T), T)

    def partner_copy(first, count):
        rows = pl.ds(pl.multiple_of(first * T, T), count * T)
        return pltpu.make_async_remote_copy(
            src_ref=sendbuf.at[rows], dst_ref=recvbuf.at[rows], send_sem=psend_sem.at[first], recv_sem=precv_sem.at[first],
            device_id=partner, device_id_type=MESH,
        )

    def finish_h(e, sums, at):
        rows = rows_of(e)
        total = ybuf[rows, :].astype(F32) + recvbuf[rows, :].astype(F32)
        h = rbuf[rows, :].astype(F32) + total
        if isinstance(e, int) and e >= ends[-1]:
            h_last[(e - ends[-1]) * T:(e - ends[-1] + 1) * T, :] = h
        else:
            hbuf[rows, :] = h
        h_out[rows, :] = h.astype(BF16)
        squares = h * h
        for b in range(per):
            block = jnp.transpose(squares[b * 128:(b + 1) * 128, :])
            sums[pl.ds(at * per + b, 1), :] = jnp.sum(block, axis=0, keepdims=True)

    def send_stage(group, stage):
        axes = STAGED[group][1][stage]
        here = 0
        for axis in axes:
            here = here * SIDE + (z, y, x)[axis]
        parts = staged_parts[group]
        for o in stage_offsets(axes):
            pltpu.make_async_remote_copy(
                src_ref=staged_sq[group].at[stage], dst_ref=parts.at[stage, here], send_sem=ssend_sem.at[group, stage],
                recv_sem=srecv_sem.at[group, stage], device_id=peer(o), device_id_type=MESH,
            ).start()
        parts[stage, here] = staged_sq[group][stage]

    def wait_stage(group, stage, sem):
        whole = staged_parts[group].at[stage, pl.ds(0, SIDE ** len(STAGED[group][1][stage]) - 1)]
        pltpu.make_async_copy(whole, whole, sem.at[group, stage]).wait()

    def stage_sums(group, stage):
        return jnp.sum(staged_parts[group][stage, 0:SIDE ** len(STAGED[group][1][stage])], axis=0)

    def next_stage(group, stage):
        wait_stage(group, stage - 1, srecv_sem)
        staged_sq[group][stage] = stage_sums(group, stage - 1)
        send_stage(group, stage)

    def staged_sums(group):
        stage = len(STAGED[group][1]) - 1
        wait_stage(group, stage, srecv_sem)
        return stage_sums(group, stage)

    def send_last():
        for o in OFFSETS:
            pltpu.make_async_remote_copy(
                src_ref=last_sq, dst_ref=last_parts.at[me], send_sem=qsend_sem, recv_sem=qrecv_sem,
                device_id=peer(o), device_id_type=MESH,
            ).start()
        last_parts[me] = last_sq[...]

    def wait_last(sem):
        whole = last_parts.at[pl.ds(0, PEERS)]
        pltpu.make_async_copy(whole, whole, sem).wait()

    def finish_n(first, sums):
        normalize(sums / width, gbuf[...], hbuf, n_out, first * T, first * T)

    def request(q):
        if isinstance(q, int):
            if q < 2 * n:
                a_copy(q).start()
        else:
            @pl.when(q < 2 * n)
            def _():
                a_copy(q).start()

    def product(q):
        return jnp.dot(abuf[q % NB], wbuf[...], preferred_element_type=F32).astype(BF16)

    def step(j, before, *places):
        request(2 * j + AHEAD + 1)
        request(2 * j + AHEAD + 2)
        a_copy(2 * j + 1).wait()
        a_copy(2 * j + 2).wait()
        before(j)
        for i, (buffer, chunk) in enumerate(places):
            buffer[rows_of(chunk), :] = product(2 * j + 1 + i)

    def loop(low, high, before=lambda j: None, after=lambda j: None):
        def body(j, _):
            step(j, before, (sendbuf, j + 1), (ybuf, j))
            after(j)
            return 0

        lax.fori_loop(low, high, body, 0)

    w_copy.wait()
    for q in range(HEAD, AHEAD + 1):
        request(q)
    a_copy(0).wait()
    sendbuf[rows_of(0), :] = product(0)
    loop(0, BARRIER_AT + 1)
    r_copy.start()
    g_copy.start()

    pl.semaphore_wait(barrier, PEERS + 1)
    first = BARRIER_AT + 2
    partner_copy(0, first).start()

    def send(j):
        partner_copy(j + 1, 1).start()

    loop(BARRIER_AT + 1, EPI_FROM, after=send)
    partner_copy(0, first).wait_recv()
    r_copy.wait()
    g_copy.wait()


    def place(e):
        for group, end in enumerate(ends):
            if e < end:
                return staged_sq[group].at[0], end - STAGED[group][0]
        return last_sq, ends[-1]

    e, j = 0, EPI_FROM
    stage_of = [None] * n_staged

    def exchange():
        for group, end in enumerate(ends):
            if stage_of[group] is not None and stage_of[group][0] < 1 and j - stage_of[group][1] >= STAGE_STEPS:
                next_stage(group, 1)
                stage_of[group] = (1, j)
            if stage_of[group] is None and e == end:
                send_stage(group, 0)
                stage_of[group] = (0, j)

    while j < n - 3:
        count = 2 if e + 2 <= j else 1
        sums, base = place(e)
        steps = 1
        while (
            j + steps < n - 3 and (2 if e + count * steps + 2 <= j + steps else 1) == count
            and place(e + count * steps)[1] == base and e + count * steps not in ends
            and (e >= first) == (e + count * steps >= first)
        ):
            steps += 1

        def before(jj, e=e, j=j, count=count, sums=sums, base=base):
            for b in range(count):
                now = e + (jj - j) * count + b
                if e + b >= first:
                    partner_copy(now, 1).wait_recv()
                elif e + b + (steps - 1) * count >= first:
                    @pl.when(now >= first)
                    def _():
                        partner_copy(now, 1).wait_recv()
                finish_h(now, sums, now - base)

        loop(j, j + steps, before=before, after=send)
        e += count * steps
        j += steps
        exchange()

    def finish_one(now):
        partner_copy(now, 1).wait_recv()
        sums, base = place(now)
        finish_h(now, sums, now - base)

    ready = e
    step(n - 3, lambda _: [finish_one(i) for i in range(ready, n - 3)], (sendbuf, n - 2), (sendbuf, n - 1))
    send(n - 3)
    send(n - 2)
    e, j = n - 3, n - 2
    exchange()
    step(n - 2, lambda _: None, (ybuf, n - 3), (ybuf, n - 2))
    j = n - 1
    exchange()
    a_copy(2 * n - 1).wait()
    finish_one(n - 3)
    finish_one(n - 2)
    ybuf[rows_of(n - 1), :] = product(2 * n - 1)
    finish_one(n - 1)
    send_last()

    for stage in range(1, max(len(stages) for _, stages in STAGED)):
        for group, (_, stages) in enumerate(STAGED):
            if stage_of[group][0] < stage < len(stages):
                next_stage(group, stage)
    for group, end in enumerate(ends):
        finish_n(end - STAGED[group][0], staged_sums(group))
    partner_copy(0, first).wait_send()
    for j in range(first, n):
        partner_copy(j, 1).wait_send()
    for group in range(n_staged):
        for stage in range(len(STAGED[group][1])):
            wait_stage(group, stage, ssend_sem)
    wait_last(qsend_sem)
    wait_last(qrecv_sem)
    sums_out[...] = jnp.sum(last_parts[...], axis=0) / width


def write_kernel(h, n, h_last, mean, gain, h_out, n_out, last_n, sem):
    early = h.shape[0] - h_last.shape[0]
    copies = [
        pltpu.make_async_copy(n.at[pl.ds(0, early)], n_out.at[pl.ds(0, early)], sem.at[0]),
        pltpu.make_async_copy(h, h_out, sem.at[1]),
    ]
    for copy in copies:
        copy.start()
    normalize(mean[...], gain[...], h_last, last_n, 0, 0)
    copies.append(pltpu.make_async_copy(last_n, n_out.at[pl.ds(early, h_last.shape[0])], sem.at[2]))
    copies[-1].start()
    for copy in copies:
        copy.wait()


def solution(mesh):
    def local_step(attn_blk, w_blk, res_blk, gain_blk):
        rows, cols = res_blk.shape
        n = rows // T
        per = T // 128
        last = (n - sum(c for c, _ in STAGED)) * per
        n_stages = max(len(stages) for _, stages in STAGED)
        hbm = pl.BlockSpec(memory_space=pltpu.HBM)
        vmem = pl.BlockSpec(memory_space=pltpu.VMEM)
        out = jax.ShapeDtypeStruct((rows, cols), BF16)
        last_rows = jax.ShapeDtypeStruct((last * 128, cols), F32)
        finished = pl.pallas_call(
            kernel,
            out_shape=(out, out, last_rows, jax.ShapeDtypeStruct((last, 128), F32), jax.ShapeDtypeStruct((1, cols), F32)),
            in_specs=[hbm] * 4,
            out_specs=(vmem,) * 5,
            scratch_shapes=[
                pltpu.VMEM((NB, T, attn_blk.shape[1]), BF16),
                pltpu.VMEM(w_blk.shape, BF16),
                pltpu.VMEM((rows, cols), BF16),
                pltpu.VMEM((rows, cols), BF16),
                pltpu.VMEM((rows, cols), BF16),
                pltpu.VMEM((rows, cols), BF16),
                pltpu.VMEM((rows, cols), F32),
                pltpu.VMEM((last, 128), F32),
                pltpu.VMEM((PEERS + 1, last, 128), F32),
                *(pltpu.VMEM((len(stages), c * per, 128), F32) for c, stages in STAGED),
                *(
                    pltpu.VMEM((len(stages), SIDE ** max(len(axes) for axes in stages), c * per, 128), F32)
                    for c, stages in STAGED
                ),
                pltpu.SemaphoreType.DMA((NB,)),
                pltpu.SemaphoreType.DMA,
                pltpu.SemaphoreType.DMA,
                pltpu.SemaphoreType.DMA,
                pltpu.SemaphoreType.DMA((n,)),
                pltpu.SemaphoreType.DMA((n,)),
                pltpu.SemaphoreType.DMA,
                pltpu.SemaphoreType.DMA,
                pltpu.SemaphoreType.DMA((len(STAGED), n_stages)),
                pltpu.SemaphoreType.DMA((len(STAGED), n_stages)),
            ],
            compiler_params=pltpu.CompilerParams(collective_id=0, has_side_effects=True, vmem_limit_bytes=40 * 2**20),
        )(*(pltpu.with_memory_space_constraint(v, pltpu.HBM) for v in (attn_blk, w_blk, res_blk, gain_blk.reshape(1, cols))))
        return pl.pallas_call(
            write_kernel,
            out_shape=(out, out),
            in_specs=[vmem] * 5,
            out_specs=(hbm, hbm),
            scratch_shapes=[pltpu.VMEM((last * 128, cols), BF16), pltpu.SemaphoreType.DMA((3,))],
            compiler_params=pltpu.CompilerParams(vmem_limit_bytes=16 * 2**20),
        )(*finished)

    row_spec = P(("dp", "tp"), "tp2")
    return jax.shard_map(
        local_step, mesh=mesh, in_specs=(P("dp", "tp"), P("tp", "tp2"), row_spec, P("tp2")),
        out_specs=(row_spec, row_spec), check_vma=False,
    )
```
